256 devices in a mesh: row: 8 (over y, x_hi), col: 32 (over z, x_lo, core).
Axes of the slice: x: 4 (x_hi: 2, x_lo: 2; x = x_hi * 2 + x_lo), y: 4, z: 8, core: 2. Of those that a mesh axis runs over, the one named last changes fastest.
Arguments:
- field: float32 [2, 2048, 16384], P(None, 'row', 'col'), may hold values from -4 to 4
- states: float32 [32, 256, 512], P('row', 'col'), may hold values from -1 to 1
- input_weight: bfloat16 [20736, 512], P('col'), may hold values from -0.0390625 to 0.0390625
- recurrent_weight: bfloat16 [512, 512], replicated, may hold values from -0.25 to 0.25
- bias: float32 [512], replicated, may hold values from -3 to 3
- output_weight: bfloat16 [512, 8192], P(None, 'col'), may hold values from -0.25 to 0.25
- model_gain: float32 [2, 64, 64], replicated, may hold values from 0.5 to 1.5
Outputs:
- prediction: float32 [2, 2048, 16384], P(None, 'row', 'col')
- fresh_states: float32 [32, 256, 512], P('row', 'col')
The draws below stay inside these ranges and needn't reach their ends.
All inputs are finite; a program needn't handle non-finite values.
Results may differ from the reference program's by a relative error of at most 0.0033.
Values may be sent and summed in bfloat16 or wider, within the bound.
A program may use at most 64 MiB of HBM per device.

```python
import jax
import jax.numpy as jnp
from jax import lax

CORE = 64
MARGIN = 4
NODES = 512
PATCH = 72
FEAT = 20736
NR = 2048
NC = 16384
BLK_ROWS = 32
BLK_COLS = 256


def level_of(rng, extent, shards, smallest, largest):
    def one(axis_at, shards_of):
        steps = jax.random.uniform(jax.random.fold_in(jax.random.fold_in(rng, 6), axis_at), (shards_of,), jnp.float32, smallest / len(shards), largest / len(shards))
        return jnp.repeat(jnp.exp(steps), extent[axis_at] // shards_of).reshape((-1,) + (1,) * (len(extent) - axis_at - 1))

    level = one(*shards[0])
    for cut in shards[1:]:
        level = level * one(*cut)
    return level


def normal_values(rng, dims, deviation, most, split=(), kind=jnp.bfloat16):
    array = jax.random.normal(rng, dims, jnp.float32) * deviation
    if len(split) > 0:
        array = level_of(rng, dims, split, -0.22, 0.18) * array
    return jnp.clip(array, min=-most, max=most).astype(kind)


def setup_inputs(seed: int = 0) -> dict:
    streams_of = jax.random.split(jax.random.key(seed), 8)
    field = normal_values(streams_of[0], (2, NR, NC), 0.6, 4.0, ((1, 8), (2, 32)), jnp.float32)
    states = jnp.clip(jax.random.uniform(streams_of[1], (BLK_ROWS, BLK_COLS, NODES), jnp.float32, -1.0, 1.0) * level_of(streams_of[1], (BLK_ROWS, BLK_COLS, NODES), ((0, 8), (1, 32)), -0.4, 0.0), -1.0, 1.0)
    input_weight = normal_values(streams_of[2], (FEAT, NODES), FEAT ** -0.5, 0.0390625, ((0, 32),))
    recurrent_weight = normal_values(streams_of[3], (NODES, NODES), NODES ** -0.5, 0.25)
    bias = normal_values(streams_of[4], (NODES,), 0.5, 3.0, (), jnp.float32)
    output_weight = normal_values(streams_of[5], (NODES, 2 * CORE * CORE), NODES ** -0.5, 0.25, ((1, 32),))
    model_gain = jnp.clip(1.0 + 0.1 * jax.random.normal(streams_of[6], (2, CORE, CORE), jnp.float32), 0.5, 1.5)
    return dict(field=field, states=states, input_weight=input_weight, recurrent_weight=recurrent_weight, bias=bias, output_weight=output_weight, model_gain=model_gain)


dispersion = 2.0
nonlinear = -0.7
time_step = 0.1


def reaction(center, spread):
    real_part = center[0]
    imag_part = center[1]
    modulus = real_part * real_part + imag_part * imag_part
    first = real_part + spread[0] - dispersion * spread[1] - modulus * (real_part - nonlinear * imag_part)
    second = imag_part + spread[1] + dispersion * spread[0] - modulus * (imag_part + nonlinear * real_part)
    return jnp.stack([first, second])


def tendency(field):
    spread = jnp.roll(field, 1, 1) + jnp.roll(field, -1, 1) + jnp.roll(field, 1, 2) + jnp.roll(field, -1, 2) - 4.0 * field
    return reaction(field, spread)


def reference(field, states, input_weight, recurrent_weight, bias, output_weight, model_gain):
    slope_one = tendency(field)
    slope_two = tendency(field + 0.5 * time_step * slope_one)
    slope_three = tendency(field + 0.5 * time_step * slope_two)
    slope_four = tendency(field + time_step * slope_three)
    model = field + time_step / 6.0 * (slope_one + 2.0 * slope_two + 2.0 * slope_three + slope_four)
    both = jnp.concatenate([field, model], 0)
    padded = jnp.pad(both, ((0, 0), (MARGIN, MARGIN), (MARGIN, MARGIN)), mode="wrap")
    starts = jnp.arange(BLK_COLS, dtype=jnp.int32) * CORE

    def one_row(index):
        slab = lax.dynamic_slice_in_dim(padded, (index * CORE).astype(jnp.int32), PATCH, 1)

        def one_patch(start):
            return lax.dynamic_slice_in_dim(slab, start.astype(jnp.int32), PATCH, 2)

        inputs = jax.vmap(one_patch)(starts).reshape(BLK_COLS, FEAT).astype(jnp.bfloat16)
        previous = lax.dynamic_index_in_dim(states, index, 0, keepdims=False).astype(jnp.bfloat16)
        drive = jnp.dot(inputs, input_weight, preferred_element_type=jnp.float32)
        recur = jnp.dot(previous, recurrent_weight, preferred_element_type=jnp.float32)
        fresh = jnp.tanh(drive + recur + bias)
        readout = jnp.dot(fresh.astype(jnp.bfloat16), output_weight, preferred_element_type=jnp.float32)
        return fresh, readout

    fresh_states, readout = lax.map(one_row, jnp.arange(BLK_ROWS, dtype=jnp.int32))
    placed = readout.reshape(BLK_ROWS, BLK_COLS, 2, CORE, CORE).transpose(2, 0, 3, 1, 4).reshape(2, NR, NC)
    gained = (model.reshape(2, BLK_ROWS, CORE, BLK_COLS, CORE) * model_gain[:, None, :, None, :]).reshape(2, NR, NC)
    prediction = gained + placed
    return prediction, fresh_states
```

```python
import jax
import jax.numpy as jnp
from jax import lax
from jax.experimental import pallas as pl
from jax.experimental.pallas import tpu as pltpu
from jax.sharding import PartitionSpec as P

CORE = 64
MARGIN = 4
NODES = 512
PATCH = 72
MESH = pl.DeviceIdType.MESH

dispersion = 2.0
nonlinear = -0.7
time_step = 0.1

TILES = 5
ROWS = 296
TOP = 20
BF = jnp.bfloat16
F32 = jnp.float32


def lane_index(rows):
    return lax.broadcasted_iota(jnp.int32, (rows, 128), 1)


def reaction(re, im, lap_re, lap_im):
    modulus = re * re + im * im
    first = re + lap_re - dispersion * lap_im - modulus * (re - nonlinear * im)
    second = im + lap_im + dispersion * lap_re - modulus * (im + nonlinear * re)
    return first, second


def forecast_kernel(
    field, patches, model,
    left_out, right_out, left_in, right_in, top_in, bottom_in, corners,
    start, ping, pong, total, main, shifted, send_sem, recv_sem,
):
    row, col = lax.axis_index("row"), lax.axis_index("col")
    up, down = lax.rem(row + 7, 8), lax.rem(row + 1, 8)
    left, right = lax.rem(col + 31, 32), lax.rem(col + 1, 32)
    around = [(up, left), (up, col), (up, right), (row, left), (row, right), (down, left), (down, col), (down, right)]
    barrier = pltpu.get_barrier_semaphore()
    for device in around:
        pl.semaphore_signal(barrier, inc=1, device_id=device, device_id_type=MESH)
    lanes = lane_index(16)
    group = lanes // 8
    for ch in range(2):
        for side, buffer in ((0, left_out), (1, right_out)):
            packed = jnp.zeros((16, 128), F32)
            for k in range(16):
                tile = field[ch, 16 * k : 16 * k + 16, 384 * side : 384 * side + 128]
                shift = (8 * k + 8 * side) % 128
                moved = tile if shift == 0 else pltpu.roll(tile, shift, 1)
                packed = jnp.where(group == k, moved, packed)
            buffer[ch] = packed
    pl.semaphore_wait(barrier, 8)

    def copy(index, source, target, device):
        return pltpu.make_async_remote_copy(
            src_ref=source, dst_ref=target, send_sem=send_sem.at[index], recv_sem=recv_sem.at[index],
            device_id=device, device_id_type=MESH,
        )

    copies = [
        copy(0, field.at[:, 0:8, 0:128], corners.at[3], around[0]),
        copy(1, field.at[:, 0:8, :], bottom_in, around[1]),
        copy(2, field.at[:, 0:8, 384:512], corners.at[2], around[2]),
        copy(3, left_out, right_in, around[3]),
        copy(4, right_out, left_in, around[4]),
        copy(5, field.at[:, 248:256, 0:128], corners.at[1], around[5]),
        copy(6, field.at[:, 248:256, :], top_in, around[6]),
        copy(7, field.at[:, 248:256, 384:512], corners.at[0], around[7]),
    ]
    for one in copies:
        one.start()
    for one in copies:
        one.wait()

    def assemble(tiles, left_tile, right_tile, lane):
        moved = [pltpu.roll(tile, 4, 1) for tile in tiles]
        first = jnp.where(lane < 4, left_tile, moved[0])
        middle = [jnp.where(lane < 4, moved[t - 1], moved[t]) for t in (1, 2, 3)]
        last = jnp.where(lane < 4, moved[3], jnp.where(lane >= 124, left_tile, right_tile))
        return [first, *middle, last]

    short = lane_index(8)
    for ch in range(2):
        for k in range(16):
            tiles = [field[ch, 16 * k : 16 * k + 16, 128 * t : 128 * t + 128] for t in range(4)]
            left_tile = pltpu.roll(left_in[ch], (-8 * k - 4) % 128, 1)
            right_shift = (4 - 8 * k) % 128
            right_tile = pltpu.roll(right_in[ch], right_shift, 1)
            for t, tile in enumerate(assemble(tiles, left_tile, right_tile, lanes)):
                start[ch, t, TOP + 16 * k : TOP + 16 * k + 16, :] = tile
        for first_row, rows, at in ((TOP - 8, top_in, 0), (TOP + 256, bottom_in, 2)):
            tiles = [rows[ch, :, 128 * t : 128 * t + 128] for t in range(4)]
            left_tile = pltpu.roll(corners[at, ch], 4, 1)
            right_tile = pltpu.roll(corners[at + 1, ch], 4, 1)
            for t, tile in enumerate(assemble(tiles, left_tile, right_tile, short)):
                start[ch, t, first_row : first_row + 8, :] = tile

    def stage(source, finish):
        def block(i, carry):
            for sub in range(5):
                at = pl.multiple_of(8 + 40 * i + 8 * sub, 8)
                center = [[source[ch, t, pl.ds(at, 8), :] for t in range(TILES)] for ch in range(2)]
                laps = []
                for ch in range(2):
                    back = [pltpu.roll(tile, 1, 1) for tile in center[ch]]
                    ahead = [pltpu.roll(tile, 127, 1) for tile in center[ch]]
                    row_laps = []
                    for t in range(TILES):
                        before = jnp.where(short == 0, back[t - 1], back[t])
                        after = jnp.where(short == 127, ahead[(t + 1) % TILES], ahead[t])
                        above = source[ch, t, pl.ds(at - 1, 8), :]
                        below = source[ch, t, pl.ds(at + 1, 8), :]
                        row_laps.append(above + below + before + after - 4.0 * center[ch][t])
                    laps.append(row_laps)
                for t in range(TILES):
                    slopes = reaction(center[0][t], center[1][t], laps[0][t], laps[1][t])
                    for ch in range(2):
                        finish((ch, t, pl.ds(at, 8)), slopes[ch])
            return carry

        lax.fori_loop(0, 7, block, 0)

    def first_stage(at, slope):
        total[at] = slope
        ping[at] = start[at] + 0.5 * time_step * slope

    def second_stage(at, slope):
        total[at] = total[at] + 2.0 * slope
        pong[at] = start[at] + 0.5 * time_step * slope

    def third_stage(at, slope):
        total[at] = total[at] + 2.0 * slope
        ping[at] = start[at] + time_step * slope

    def fourth_stage(at, slope):
        pong[at] = start[at] + time_step / 6.0 * (total[at] + slope)

    stage(start, first_stage)
    stage(ping, second_stage)
    stage(pong, third_stage)
    stage(ping, fourth_stage)

    for channel in range(4):
        source, ch = (start, channel) if channel < 2 else (pong, channel - 2)

        def gather(i, carry):
            for a in range(4):
                at = pl.multiple_of(64 * a + 16 + 8 * i, 8)
                tiles = [source[ch, t, pl.ds(at, 8), :] for t in range(TILES)]
                for j in range(4):
                    main[pl.ds(128 * i + 4 * a + j, 8, stride=16), :] = tiles[j]
                    shifted[pl.ds(128 * i + 4 * a + j, 8, stride=16), :] = tiles[j + 1]
            return carry

        lax.fori_loop(0, 9, gather, 0)

        def pack(q, carry):
            at = pl.multiple_of(144 * q, 16)
            patches[8 * channel + q, 0:9] = main[pl.ds(at, 144), :].reshape(9, 16, 128).astype(BF)
            tail = jnp.zeros((16, 128), F32)
            for y in range(9):
                tile = shifted[pl.ds(pl.multiple_of(at + 16 * y, 16), 16), :]
                moved = tile if y == 0 else pltpu.roll(tile, 8 * y, 1)
                tail = jnp.where(group == y, moved, tail)
            patches[8 * channel + q, 9] = tail.astype(BF)
            return carry

        lax.fori_loop(0, 8, pack, 0)

    for ch in range(2):
        for k in range(16):
            tiles = [pltpu.roll(pong[ch, t, TOP + 16 * k : TOP + 16 * k + 16, :], 124, 1) for t in range(TILES)]
            for t in range(4):
                model[ch, 16 * k : 16 * k + 16, 128 * t : 128 * t + 128] = jnp.where(lanes < 124, tiles[t], tiles[t + 1])


def forecast(field):
    vmem = pl.BlockSpec(memory_space=pltpu.VMEM)
    block = pltpu.VMEM((2, TILES, ROWS, 128), F32)
    return pl.pallas_call(
        forecast_kernel,
        name="forecast",
        out_shape=(
            jax.ShapeDtypeStruct((32, 10, 16, 128), BF),
            jax.ShapeDtypeStruct((2, 256, 512), F32),
        ),
        in_specs=[vmem],
        out_specs=(vmem, vmem),
        scratch_shapes=[
            pltpu.VMEM((2, 16, 128), F32),
            pltpu.VMEM((2, 16, 128), F32),
            pltpu.VMEM((2, 16, 128), F32),
            pltpu.VMEM((2, 16, 128), F32),
            pltpu.VMEM((2, 8, 512), F32),
            pltpu.VMEM((2, 8, 512), F32),
            pltpu.VMEM((4, 2, 8, 128), F32),
            block,
            block,
            block,
            block,
            pltpu.VMEM((1152, 128), F32),
            pltpu.VMEM((1152, 128), F32),
            pltpu.SemaphoreType.DMA((8,)),
            pltpu.SemaphoreType.DMA((8,)),
        ],
        compiler_params=pltpu.CompilerParams(collective_id=0, has_side_effects=True),
    )(field)


def reservoir_kernel(
    patches, model, win, wout, wrec, bias, states, gain,
    prediction, fresh,
    rows, weights, wide, readout_weights, arrived, partial, partials, mine, readin, pieces, returned, placed,
    z_send, z_recv, z_local, d2d_send, d2d_recv, in_send, in_recv, drive_send, drive_recv,
    readin_send, readin_recv, out_send, out_recv,
):
    row, col = lax.axis_index("row"), lax.axis_index("col")
    z, x_lo, core = col // 4, lax.rem(col // 2, 2), lax.rem(col, 2)
    me = 2 * row + x_lo
    other_core = (row, col + 1 - 2 * core)
    hop = lax.rem(row + 4 * core, 8)
    z_source, z_target = lax.rem(z + hop, 8), lax.rem(z + 8 - hop, 8)
    source_device = (row, 4 * z_source + 2 * x_lo + core)
    target_device = (row, 4 * z_target + 2 * x_lo + core)

    def peer(i):
        index = lax.rem(me + i, 16)
        return index, (index // 2, 4 * z + 2 * lax.rem(index, 2) + core)

    def shard(index, kind):
        plane = lax.rem(z + index // 2 + 4 * kind, 8)
        return 4 * plane + 2 * lax.rem(index, 2) + kind

    barrier = pltpu.get_barrier_semaphore()

    def greet(i, carry):
        _, device = peer(i)
        pl.semaphore_signal(barrier, inc=1, device_id=device, device_id_type=MESH)
        return carry

    lax.fori_loop(1, 16, greet, 0)
    pl.semaphore_signal(barrier, inc=1, device_id=other_core, device_id_type=MESH)

    @pl.when(hop != 0)
    def _():
        pl.semaphore_signal(barrier, inc=1, device_id=source_device, device_id_type=MESH)
        pl.semaphore_signal(barrier, inc=1, device_id=target_device, device_id_type=MESH)

    pl.semaphore_wait(barrier, 16 + 2 * jnp.minimum(hop, 1))

    def remote(source, target, send_sem, recv_sem, device):
        return pltpu.make_async_remote_copy(
            src_ref=source, dst_ref=target, send_sem=send_sem, recv_sem=recv_sem, device_id=device, device_id_type=MESH
        )

    z_copies = [
        remote(win, weights.at[core], z_send.at[0], z_recv.at[0], target_device),
        remote(wout, readout_weights.at[core], z_send.at[1], z_recv.at[1], target_device),
    ]
    own_copies = [
        pltpu.make_async_copy(win, weights.at[core], z_local.at[0]),
        pltpu.make_async_copy(wout, readout_weights.at[core], z_local.at[1]),
    ]

    @pl.when(hop != 0)
    def _():
        for one in z_copies:
            one.start()

    @pl.when(hop == 0)
    def _():
        for one in own_copies:
            one.start()

    def in_copy(kind, source, slot, device):
        return remote(source, arrived.at[kind, :, slot], in_send.at[kind, slot], in_recv.at[kind, slot], device)

    def send_inputs(i, carry):
        index, device = peer(i)
        for kind in range(2):
            remote(
                patches.at[shard(index, kind)], arrived.at[kind, :, me], in_send.at[kind, index], in_recv.at[kind, me], device
            ).start()
        return carry

    lax.fori_loop(1, 16, send_inputs, 0)
    for kind in range(2):
        arrived[kind, :, me] = patches[shard(me, kind)]

    wide[...] = jnp.zeros(wide.shape, BF)
    recur = []
    for t in range(4):
        rows[t] = states[:, 128 * t : 128 * t + 128]
    for p in range(2):
        before = jnp.concatenate([rows[t, pl.ds(p, 16, stride=2), :] for t in range(4)], axis=1).astype(BF)
        recur.append(jnp.dot(before, wrec[...], preferred_element_type=F32) + bias[...])

    @pl.when(hop != 0)
    def _():
        for one in z_copies:
            one.wait()

    @pl.when(hop == 0)
    def _():
        for one in own_copies:
            one.wait()

    d2d_copies = [
        remote(weights.at[core], weights.at[core], d2d_send.at[0], d2d_recv.at[0], other_core),
        remote(readout_weights.at[core], readout_weights.at[core], d2d_send.at[1], d2d_recv.at[1], other_core),
    ]
    for one in d2d_copies:
        one.start()
    for one in d2d_copies:
        one.wait()

    for kind in range(2):
        tails = []
        for y in range(9):
            block = weights[kind, y]
            wide[10 * kind + y, 0:72, 0:512] = block
            wide[10 * kind + y, 64:128, 512:1024] = block[0:64]
            tails.append(block[64:72].astype(F32))
        tails.append(jnp.zeros((56, 512), F32))
        wide[10 * kind + 9, :, 512:1024] = jnp.concatenate(tails, axis=0).astype(BF)

    def wait_inputs(i, carry):
        index, device = peer(i)
        for kind in range(2):
            remote(
                patches.at[0], arrived.at[kind, :, index], in_send.at[kind, index], in_recv.at[kind, index], device
            ).wait()
        return carry

    lax.fori_loop(1, 16, wait_inputs, 0)
    left_side = jnp.concatenate([arrived[kind, y].reshape(256, 128) for kind in range(2) for y in range(10)], axis=1)
    for n in range(4):
        right_side = wide[:, :, 256 * n : 256 * n + 256].reshape(2560, 256)
        part = jnp.dot(left_side, right_side, preferred_element_type=F32)
        partial[:, :, 256 * n : 256 * n + 256] = part.astype(BF).reshape(16, 16, 256)

    def send_drives(i, carry):
        index, device = peer(i)
        remote(partial.at[index], partials.at[me], drive_send.at[index], drive_recv.at[me], device).start()
        return carry

    lax.fori_loop(1, 16, send_drives, 0)
    partials[me] = partial[me]

    def wait_drives(i, carry):
        index, device = peer(i)
        remote(partial.at[index], partials.at[index], drive_send.at[index], drive_recv.at[index], device).wait()
        return carry

    lax.fori_loop(1, 16, wait_drives, 0)
    drive = partials[0].astype(F32)
    for index in range(1, 16):
        drive = drive + partials[index].astype(F32)
    for p in range(2):
        state = jnp.tanh(drive[:, 512 * p : 512 * p + 512] + recur[p])
        for t in range(4):
            rows[t, pl.ds(p, 16, stride=2), :] = state[:, 128 * t : 128 * t + 128]
        mine[p] = state.astype(BF)
    for t in range(4):
        fresh[:, 128 * t : 128 * t + 128] = rows[t]

    def send_readin(i, carry):
        index, device = peer(i)
        remote(mine, readin.at[:, me], readin_send.at[index], readin_recv.at[me], device).start()
        return carry

    lax.fori_loop(1, 16, send_readin, 0)
    readin[:, me] = mine[...]

    def wait_readin(i, carry):
        index, device = peer(i)
        remote(mine, readin.at[:, index], readin_send.at[index], readin_recv.at[index], device).wait()
        return carry

    lax.fori_loop(1, 16, wait_readin, 0)
    half = lane_index(256) < 64
    for kind in range(2):
        out = [
            jnp.dot(readin[p].reshape(256, 512), readout_weights[kind], preferred_element_type=F32) for p in range(2)
        ]
        for pair in range(2):
            even, odd = (value[:, 128 * pair : 128 * pair + 128] for value in out)
            first = jnp.where(half, even, pltpu.roll(odd, 64, 1))
            second = jnp.where(half, pltpu.roll(even, 64, 1), odd)
            pieces[:, kind, 2 * pair] = first.astype(BF).reshape(16, 16, 128)
            pieces[:, kind, 2 * pair + 1] = second.astype(BF).reshape(16, 16, 128)

    def send_out(i, carry):
        index, device = peer(i)
        for kind in range(2):
            remote(
                pieces.at[index, kind], returned.at[shard(me, kind)], out_send.at[kind, index], out_recv.at[kind, me], device
            ).start()
        return carry

    lax.fori_loop(1, 16, send_out, 0)
    for kind in range(2):
        returned[shard(me, kind)] = pieces[me, kind]

    def wait_out(i, carry):
        index, device = peer(i)
        for kind in range(2):
            remote(
                pieces.at[index, kind], returned.at[shard(index, kind)], out_send.at[kind, index], out_recv.at[kind, index], device
            ).wait()
        return carry

    lax.fori_loop(1, 16, wait_out, 0)
    for ch in range(2):

        def place(k, carry):
            for y in range(4):
                tile = returned[16 * ch + k, y].astype(F32)
                placed[ch, pl.ds(4 * k + y, 16, stride=64), :] = tile
            return carry

        lax.fori_loop(0, 16, place, 0)
        for a in range(4):
            for j in range(4):
                at = (slice(64 * a, 64 * a + 64), slice(128 * j, 128 * j + 128))
                base = 64 * (4 * a + j)
                prediction[(ch, *at)] = gain[ch] * model[(ch, *at)] + placed[ch, base : base + 64, :]


def reservoir(patches, model, win, wout, wrec, bias, states, gain):
    vmem = pl.BlockSpec(memory_space=pltpu.VMEM)
    hbm = pl.BlockSpec(memory_space=pl.ANY)
    dma = pltpu.SemaphoreType.DMA
    return pl.pallas_call(
        reservoir_kernel,
        name="reservoir",
        out_shape=(
            jax.ShapeDtypeStruct((2, 256, 512), F32),
            jax.ShapeDtypeStruct((32, 512), F32),
        ),
        in_specs=[vmem, vmem, hbm, hbm, vmem, vmem, vmem, vmem],
        out_specs=(vmem, vmem),
        scratch_shapes=[
            pltpu.VMEM((4, 32, 128), F32),
            pltpu.VMEM((2, 9, 72, 512), BF),
            pltpu.VMEM((20, 128, 1024), BF),
            pltpu.VMEM((2, 512, 256), BF),
            pltpu.VMEM((2, 10, 16, 16, 128), BF),
            pltpu.VMEM((16, 16, 1024), BF),
            pltpu.VMEM((16, 16, 1024), BF),
            pltpu.VMEM((2, 16, 512), BF),
            pltpu.VMEM((2, 16, 16, 512), BF),
            pltpu.VMEM((16, 2, 4, 16, 128), BF),
            pltpu.VMEM((32, 4, 16, 128), BF),
            pltpu.VMEM((2, 1024, 128), F32),
            dma((2,)), dma((2,)), dma((2,)),
            dma((2,)), dma((2,)),
            dma((2, 16)), dma((2, 16)),
            dma((16,)), dma((16,)),
            dma((16,)), dma((16,)),
            dma((2, 16)), dma((2, 16)),
        ],
        compiler_params=pltpu.CompilerParams(collective_id=1, has_side_effects=True, vmem_limit_bytes=48 << 20),
    )(patches, model, win, wout, wrec, bias, states, gain)


def local(field, states, input_weight, recurrent_weight, bias, output_weight, model_gain):
    patches, model = forecast(field)
    gain = jnp.concatenate([model_gain, model_gain], axis=2)
    prediction, fresh = reservoir(
        patches, model, input_weight.reshape(9, PATCH, NODES), output_weight, recurrent_weight,
        bias.reshape(1, NODES), states.reshape(32, NODES), gain,
    )
    return prediction, fresh.reshape(4, 8, NODES)


def solution(mesh):
    placed = (
        P(None, "row", "col"),
        P("row", "col", None),
        P("col", None),
        P(),
        P(),
        P(None, "col"),
        P(),
    )
    return jax.shard_map(
        local, mesh=mesh, in_specs=placed, out_specs=(P(None, "row", "col"), P("row", "col", None)), check_vma=False
    )
```
